1024 devices in a mesh: grp: 16 (over z), ep: 64 (over y, x, core).
Axes of the slice: x: 4, y: 8, z: 16, core: 2. Of those that a mesh axis runs over, the one named last changes fastest.
Arguments:
- hidden: bfloat16 [16, 64, 256, 1024], P('grp', 'ep'), may hold values from -6 to 6
- down_weight: bfloat16 [64, 1024, 4096], P('ep'), may hold values from -0.1875 to 0.1875
- slot_gate: float32 [16, 64, 256], P('grp', 'ep'), may hold values from 0.02 to 0.6
- slot_owner: int32 [16, 64, 256], P('grp', 'ep'), may hold values from 0 to 15
- slot_row: int32 [16, 64, 256], P('grp', 'ep'), may hold values from 0 to 31
- block_count: int32 [16, 64, 64], P('grp', 'ep'), may hold values from 0 to 4, as said below
Outputs:
- mixed: bfloat16 [32768, 4096], P(('grp', 'ep'))
The draws below stay inside these ranges and needn't reach their ends.
Inputs may be any that keep to these rules, and one draw needn't show every extreme that they name: `block_count`: every device's expert has at least one block with all 4 slots live.
All inputs are finite; a program needn't handle non-finite values.
Results may differ from the reference program's by a relative error of at most 0.009.
Values may be sent and summed in bfloat16 or wider, within the bound.
No kernel may reach another device: no remote copies, remote signals or barrier semaphores. Data moves between devices by JAX's collectives and lax.ppermute only.
A program may use at most 64 MiB of HBM per device.

```python
import math
import jax
import jax.numpy as jnp
from jax import lax

D = 4096
FFW = 1024
TOK_DEV = 32
SEND = 4
EXPERTS = 64
GROUPS = 16
COLUMNS = 64
SLOTS = 256
TOKENS = 32768
N_EP = 64


def draw_block_count(key, part):
    base = jax.random.randint(jax.random.fold_in(key, 11), (GROUPS, EXPERTS, COLUMNS), 0, SEND + 1)
    chosen = jax.random.randint(jax.random.fold_in(key, 12), (GROUPS, EXPERTS, 1), 0, COLUMNS)
    places = jnp.arange(COLUMNS).astype(jnp.int32)[None, None, :]
    return jnp.where(places == chosen, SEND, base).astype(jnp.int32)


def place_ends(result, stream_key, smallest, top_value):
    index_at = [jax.random.randint(jax.random.fold_in(stream_key, axis), (), 0, length) for axis, length in enumerate(result.shape)]
    widest = result.shape.index(max(result.shape))
    neighbour = index_at[:widest] + [(index_at[widest] + 1) % result.shape[widest]] + index_at[widest + 1:]
    return result.at[tuple(index_at)].set(smallest).at[tuple(neighbour)].set(top_value)


def shard_levels(rng, extent, pieces, smallest, high):
    def one(dim, shards_of):
        draws = jax.random.uniform(jax.random.fold_in(jax.random.fold_in(rng, 6), dim), (shards_of,), jnp.float32, smallest / len(pieces), high / len(pieces))
        return jnp.repeat(jnp.exp(draws), extent[dim] // shards_of).reshape((-1,) + (1,) * (len(extent) - dim - 1))

    gain = one(*pieces[0])
    for cut in pieces[1:]:
        gain = gain * one(*cut)
    return gain


def normal_values(rng, extent, width, bound, pieces=(), dtype=jnp.bfloat16):
    factor_of = shard_levels(rng, extent, pieces, -0.22, 0.18) if pieces else 1.0
    result = jax.random.normal(rng, extent, jnp.float32) * width * factor_of
    return jnp.minimum(jnp.maximum(result, -bound), bound).astype(dtype)


def setup_inputs(seed: int = 0) -> dict:
    key_of = jax.random.split(jax.random.key(seed), 7)
    hidden = normal_values(key_of[0], (GROUPS, EXPERTS, SLOTS, FFW), 1.0, 6.0, ((0, 16), (1, 64)))
    down_weight = normal_values(key_of[1], (EXPERTS, FFW, D), FFW ** -0.5, 0.1875, ((0, 64),))
    slot_gate = jnp.clip(jnp.exp(math.log(0.6) - 3.4011974 * jax.random.uniform(key_of[2], (GROUPS, EXPERTS, SLOTS), jnp.float32) ** shard_levels(key_of[2], (GROUPS, EXPERTS, SLOTS), ((0, 16), (1, 64)), -0.2, 0.2)), 0.02, 0.6)
    slot_owner = place_ends(jax.random.randint(key_of[3], (GROUPS, EXPERTS, SLOTS), 0, GROUPS), jax.random.fold_in(key_of[3], 1), 0, GROUPS - 1).astype(jnp.int32)
    slot_row = place_ends(jax.random.randint(key_of[4], (GROUPS, EXPERTS, SLOTS), 0, TOK_DEV), jax.random.fold_in(key_of[4], 1), 0, TOK_DEV - 1).astype(jnp.int32)
    block_count = draw_block_count(jax.random.fold_in(key_of[6], 71), 0)
    return {"hidden": hidden, "down_weight": down_weight, "slot_gate": slot_gate, "slot_owner": slot_owner, "slot_row": slot_row, "block_count": block_count}


def reference(hidden, down_weight, slot_gate, slot_owner, slot_row, block_count):
    column = (jnp.arange(SLOTS) // SEND).astype(jnp.int32)
    within = (jnp.arange(SLOTS) % SEND).astype(jnp.int32)

    def expert_rows(pair):
        rows_in, weight = pair
        return jnp.dot(rows_in, weight, preferred_element_type=jnp.float32)

    def group_step(total, inputs):
        group_hidden, gates, owners, row_index, counts = inputs
        product = lax.map(expert_rows, (group_hidden, down_weight))
        live = (within[None, :] < counts[:, column]).astype(jnp.float32)
        scale = gates * live
        sent = (product * scale[:, :, None]).astype(jnp.bfloat16)
        token = ((owners * N_EP + column[None, :]) * TOK_DEV + row_index).astype(jnp.int32)
        summed = jax.ops.segment_sum(sent.reshape(-1, D).astype(jnp.float32), token.reshape(-1), num_segments=TOKENS)
        rounded = lax.optimization_barrier(summed.astype(jnp.bfloat16))
        return total + rounded.astype(jnp.float32), None

    start = jnp.zeros((TOKENS, D), jnp.float32)
    total, unused = lax.scan(group_step, start, (hidden, slot_gate, slot_owner, slot_row, block_count))
    return total.astype(jnp.bfloat16)
```

```python
import jax
import jax.numpy as jnp
from jax import lax
from jax.sharding import PartitionSpec as P

TOK_DEV = 32


def body(hidden, down_weight, slot_gate, slot_owner, slot_row, block_count):
    planes = lax.axis_size("grp")
    columns = lax.axis_size("ep")
    per_plane = columns // planes
    slot_total = hidden.shape[2]
    width = down_weight.shape[2]
    send = slot_total // columns
    bundle = slot_total // planes
    strip = width // planes
    tokens = planes * TOK_DEV

    within = jnp.arange(slot_total) % send
    limits = jnp.repeat(block_count[0, 0], send)
    live = (within < limits).astype(jnp.float32)
    scale = slot_gate[0, 0] * live
    index = slot_owner[0, 0] * TOK_DEV + slot_row[0, 0]

    rows = lax.all_to_all(hidden[0, 0], "grp", split_axis=0, concat_axis=0, tiled=True)
    notes = jnp.concatenate(
        [scale.reshape(planes, bundle), index.astype(jnp.float32).reshape(planes, bundle)], axis=1
    )
    notes = lax.all_to_all(notes, "grp", split_axis=0, concat_axis=0, tiled=True)

    def by_column(value):
        return value.reshape((planes, per_plane, send) + value.shape[2:]).swapaxes(0, 1)

    scale = by_column(notes[:, :bundle]).reshape(slot_total)
    index = by_column(notes[:, bundle:]).reshape(per_plane, planes * send)
    index = jnp.broadcast_to(index[None], (planes, per_plane, planes * send)).reshape(columns, planes * send)
    index = lax.all_to_all(index, "ep", split_axis=0, concat_axis=0, tiled=True).reshape(-1)

    rows = by_column(rows.reshape(planes, bundle, -1)).reshape(slot_total, -1)
    product = jnp.dot(rows, down_weight[0], preferred_element_type=jnp.float32)
    scaled = (product * scale[:, None]).astype(jnp.bfloat16)
    scaled = scaled.reshape(slot_total, planes, strip).swapaxes(0, 1).reshape(planes * slot_total, strip)
    arrived = lax.all_to_all(scaled, "ep", split_axis=0, concat_axis=0, tiled=True)

    wanted = jnp.arange(tokens).astype(jnp.float32)
    table = (wanted[:, None] == index[None, :]).astype(jnp.bfloat16)
    summed = jnp.dot(table, arrived, preferred_element_type=jnp.float32).astype(jnp.bfloat16)

    summed = lax.all_to_all(summed, "grp", split_axis=0, concat_axis=0, tiled=True)
    siblings = [[d * per_plane + k for d in range(planes)] for k in range(per_plane)]
    summed = lax.all_to_all(summed, "ep", split_axis=0, concat_axis=0, tiled=True, axis_index_groups=siblings)
    return summed.reshape(planes, TOK_DEV, strip).swapaxes(0, 1).reshape(TOK_DEV, width)


def solution(mesh):
    in_specs = (
        P("grp", "ep", None, None),
        P("ep", None, None),
        P("grp", "ep", None),
        P("grp", "ep", None),
        P("grp", "ep", None),
        P("grp", "ep", None),
    )
    out_specs = P(("grp", "ep"), None)
    return jax.shard_map(body, mesh=mesh, in_specs=in_specs, out_specs=out_specs, check_vma=False)
```

```python
import jax
import jax.numpy as jnp
from jax import lax
from jax.experimental import pallas as pl
from jax.experimental.pallas import tpu as pltpu
from jax.sharding import PartitionSpec as P

TOK_DEV = 32


def exchange(value, axis, groups=None):
    return lax.all_to_all(value, axis, split_axis=0, concat_axis=0, tiled=True, axis_index_groups=groups)


def scale_kernel(send, gate_ref, count_ref, hidden_ref, out_ref):
    slots, columns = hidden_ref.shape[0], count_ref.shape[1]
    slot = lax.broadcasted_iota(jnp.int32, (slots, 1), 0)
    own = slot == lax.broadcasted_iota(jnp.int32, (slots, slots), 1)
    gate = jnp.sum(jnp.where(own, gate_ref[...], 0.0), axis=1, keepdims=True)
    block = slot // send == lax.broadcasted_iota(jnp.int32, (slots, columns), 1)
    limit = jnp.sum(jnp.where(block, count_ref[...], 0).astype(jnp.float32), axis=1, keepdims=True)
    scale = jnp.where((slot % send).astype(jnp.float32) < limit, gate, 0.0)
    out_ref[...] = (hidden_ref[...].astype(jnp.float32) * scale).astype(jnp.bfloat16)


def scaled_rows(hidden, gate, count, send):
    return pl.pallas_call(
        lambda *refs: scale_kernel(send, *refs),
        out_shape=jax.ShapeDtypeStruct(hidden.shape, jnp.bfloat16),
        cost_estimate=pl.CostEstimate(flops=2 * hidden.size, bytes_accessed=4 * hidden.size, transcendentals=0),
        name="scaled_rows",
    )(gate, count, hidden)


def product_kernel(strip, mates, send, rows_ref, weight_ref, out_ref, sorted_ref):
    count = rows_ref.shape[0]
    block = out_ref.shape[0] // count * strip

    @pl.when(pl.program_id(0) == 0)
    def _():
        place = lax.broadcasted_iota(jnp.int32, (count, count), 0)
        source = lax.broadcasted_iota(jnp.int32, (count, count), 1)
        groups = count // (mates * send)
        mate, group, slot = place // (groups * send), (place // send) % groups, place % send
        move = (source == (group * mates + mate) * send + slot).astype(jnp.float32).astype(jnp.bfloat16)
        sorted_ref[...] = jnp.dot(move, rows_ref[...], preferred_element_type=jnp.float32).astype(jnp.bfloat16)

    product = jnp.dot(sorted_ref[...], weight_ref[...], preferred_element_type=jnp.float32).astype(jnp.bfloat16)
    for i in range(block // strip):
        out_ref[i * count : (i + 1) * count, :] = product[:, i * strip : (i + 1) * strip]


def strip_product(rows, weight, strip, mates, send):
    count, depth = rows.shape
    width = weight.shape[1]
    block = 2 * strip
    return pl.pallas_call(
        lambda *refs: product_kernel(strip, mates, send, *refs),
        grid=(width // block,),
        out_shape=jax.ShapeDtypeStruct((width // strip * count, strip), jnp.bfloat16),
        in_specs=[pl.BlockSpec(memory_space=pltpu.VMEM), pl.BlockSpec((depth, block), lambda i: (0, i))],
        out_specs=pl.BlockSpec((block // strip * count, strip), lambda i: (i, 0)),
        scratch_shapes=[pltpu.VMEM((count, depth), jnp.bfloat16)],
        cost_estimate=pl.CostEstimate(
            flops=2 * count * depth * width, bytes_accessed=2 * (depth + count) * width, transcendentals=0
        ),
        name="strip_product",
    )(rows, weight)


def body(hidden, down_weight, slot_gate, slot_owner, slot_row, block_count):
    planes = lax.axis_size("grp")
    columns = lax.axis_size("ep")
    slot_total, _ = hidden.shape[2:]
    width = down_weight.shape[2]
    mates = columns // planes
    send = slot_total // columns
    strip = width // planes
    tokens = planes * TOK_DEV

    rows = scaled_rows(hidden[0, 0], slot_gate[0], block_count[0], send)
    rows = exchange(rows, "grp")

    mate = lax.axis_index("ep") % mates
    index = slot_owner[0, 0] * TOK_DEV + slot_row[0, 0]
    index = lax.all_gather(index, "ep", axis=0)
    index = index.reshape(columns, planes, mates, send)
    index = lax.dynamic_index_in_dim(index, mate, axis=2, keepdims=False).swapaxes(0, 1)
    index = index.reshape(planes, columns * send)

    product = strip_product(rows, down_weight[0], strip, mates, send)
    arrived = exchange(product, "ep")

    index = lax.all_gather(index, "grp", axis=0)
    index = lax.dynamic_index_in_dim(index, lax.axis_index("grp"), axis=1, keepdims=False)
    index = index.reshape(planes, columns, send).swapaxes(0, 1).reshape(-1)

    wanted = jnp.arange(tokens)
    table = (wanted[:, None] == index[None, :]).astype(jnp.bfloat16)
    summed = jnp.dot(table, arrived, preferred_element_type=jnp.float32).astype(jnp.bfloat16)

    summed = exchange(summed, "grp")
    siblings = [[d * mates + k for d in range(planes)] for k in range(mates)]
    summed = exchange(summed, "ep", siblings)
    return summed.reshape(planes, TOK_DEV, strip).swapaxes(0, 1).reshape(TOK_DEV, width)


def solution(mesh):
    in_specs = (
        P("grp", "ep", None, None),
        P("ep", None, None),
        P("grp", "ep", None),
        P("grp", "ep", None),
        P("grp", "ep", None),
        P("grp", "ep", None),
    )
    out_specs = P(("grp", "ep"), None)
    return jax.shard_map(body, mesh=mesh, in_specs=in_specs, out_specs=out_specs, check_vma=False)
```

```python
import jax
import jax.numpy as jnp
from jax import lax
from jax.experimental import pallas as pl
from jax.experimental.pallas import tpu as pltpu
from jax.sharding import PartitionSpec as P

TOK_DEV = 32


def exchange(value, axis, groups=None):
    return lax.all_to_all(value, axis, split_axis=0, concat_axis=0, tiled=True, axis_index_groups=groups)


def moved(rows, source):
    pick = source == lax.broadcasted_iota(jnp.int32, source.shape, 1)
    pick = pick.astype(jnp.float32).astype(jnp.bfloat16)
    return jnp.dot(pick, rows, preferred_element_type=jnp.float32).astype(jnp.bfloat16)


def scale_kernel(planes, mates, send, gate_ref, count_ref, hidden_ref, out_ref):
    slots, columns = hidden_ref.shape[0], count_ref.shape[1]
    slot = lax.broadcasted_iota(jnp.int32, (slots, 1), 0)
    own = slot == lax.broadcasted_iota(jnp.int32, (slots, slots), 1)
    gate = jnp.sum(jnp.where(own, gate_ref[...], 0.0), axis=1, keepdims=True)
    block = slot // send == lax.broadcasted_iota(jnp.int32, (slots, columns), 1)
    limit = jnp.sum(jnp.where(block, count_ref[...], 0).astype(jnp.float32), axis=1, keepdims=True)
    scale = jnp.where((slot % send).astype(jnp.float32) < limit, gate, 0.0)
    scaled = (hidden_ref[...].astype(jnp.float32) * scale).astype(jnp.bfloat16)
    place = lax.broadcasted_iota(jnp.int32, (slots, slots), 0)
    plane, mate, slot = place // (mates * send), (place // send) % mates, place % send
    out_ref[...] = moved(scaled, (mate * planes + plane) * send + slot)


def scaled_rows(hidden, gate, count, planes, mates, send):
    return pl.pallas_call(
        lambda *refs: scale_kernel(planes, mates, send, *refs),
        out_shape=jax.ShapeDtypeStruct(hidden.shape, jnp.bfloat16),
        cost_estimate=pl.CostEstimate(flops=2 * hidden.size, bytes_accessed=4 * hidden.size, transcendentals=0),
        name="scaled_rows",
    )(gate, count, hidden)


def product_kernel(planes, mates, send, rows_ref, weight_ref, out_ref, weights, outs, in_sems, out_sems):
    count = rows_ref.shape[0]
    pieces, _, block = weights.shape
    strip = out_ref.shape[3]
    per = block // strip
    loads = [
        pltpu.make_async_copy(weight_ref.at[:, i * block : (i + 1) * block], weights.at[i], in_sems.at[i])
        for i in range(pieces)
    ]
    stores = [
        pltpu.make_async_copy(outs.at[:, i * per : (i + 1) * per], out_ref.at[:, i * per : (i + 1) * per], out_sems.at[i])
        for i in range(pieces)
    ]
    for load in loads:
        load.start()
    place = lax.broadcasted_iota(jnp.int32, (count, count), 0)
    mate, group, slot = place // (planes * send), (place // send) % planes, place % send
    rows = moved(rows_ref[...], (group * mates + mate) * send + slot)
    bundle = planes * send
    for i in range(pieces):
        loads[i].wait()
        product = jnp.dot(rows, weights[i], preferred_element_type=jnp.float32).astype(jnp.bfloat16)
        for j in range(per):
            for k in range(mates):
                outs[k, i * per + j] = product[k * bundle : (k + 1) * bundle, j * strip : (j + 1) * strip]
        if i:
            stores[i - 1].start()
    stores[-1].start()
    for store in stores:
        store.wait()


def strip_product(rows, weight, planes, mates, send):
    count, depth = rows.shape
    width = weight.shape[1]
    strip = width // planes
    block = 2 * strip
    pieces = width // block
    shape = (mates, planes, planes * send, strip)
    return pl.pallas_call(
        lambda *refs: product_kernel(planes, mates, send, *refs),
        out_shape=jax.ShapeDtypeStruct(shape, jnp.bfloat16),
        in_specs=[pl.BlockSpec(memory_space=pltpu.VMEM), pl.BlockSpec(memory_space=pltpu.HBM)],
        out_specs=pl.BlockSpec(memory_space=pltpu.HBM),
        scratch_shapes=[
            pltpu.VMEM((pieces, depth, block), jnp.bfloat16),
            pltpu.VMEM(shape, jnp.bfloat16),
            pltpu.SemaphoreType.DMA((pieces,)),
            pltpu.SemaphoreType.DMA((pieces,)),
        ],
        cost_estimate=pl.CostEstimate(
            flops=2 * count * depth * width, bytes_accessed=2 * (depth + count) * width, transcendentals=0
        ),
        compiler_params=pltpu.CompilerParams(vmem_limit_bytes=50 * 1024 * 1024),
        name="strip_product",
    )(rows, weight)


def gathered(index):
    columns = lax.axis_size("ep")
    near = min(8, columns // 2)
    groups = [[i * near + j for j in range(near)] for i in range(columns // near)]
    index = lax.all_gather(index, "ep", axis=0, axis_index_groups=groups)
    step = near
    while step < columns:
        upper = (lax.axis_index("ep") // step) % 2 == 1
        other = lax.ppermute(index, "ep", [(i, i ^ step) for i in range(columns)])
        low, high = jnp.where(upper, other, index), jnp.where(upper, index, other)
        index = jnp.concatenate([low, high], axis=0)
        step *= 2
    return index


def body(hidden, down_weight, slot_gate, slot_owner, slot_row, block_count):
    planes = lax.axis_size("grp")
    columns = lax.axis_size("ep")
    slot_total = hidden.shape[2]
    width = down_weight.shape[2]
    mates = columns // planes
    send = slot_total // columns
    strip = width // planes
    tokens = planes * TOK_DEV

    rows = scaled_rows(hidden[0, 0], slot_gate[0], block_count[0], planes, mates, send)
    rows = exchange(rows, "grp")

    index = slot_owner[0, 0] * TOK_DEV + slot_row[0, 0]
    index = gathered(index).reshape(columns, mates, planes, send)
    index = lax.dynamic_index_in_dim(index, lax.axis_index("ep") // planes, axis=1, keepdims=False)
    index = index.swapaxes(0, 1).reshape(planes, columns * send)

    product = strip_product(rows, down_weight[0], planes, mates, send)
    arrived = exchange(product.reshape(columns * planes * send, strip), "ep")

    index = lax.all_gather(index, "grp", axis=0)
    index = lax.dynamic_index_in_dim(index, lax.axis_index("grp"), axis=1, keepdims=False)
    index = index.reshape(planes, columns, send).swapaxes(0, 1).reshape(-1)

    wanted = jnp.arange(tokens)
    table = (wanted[:, None] == index[None, :]).astype(jnp.bfloat16)
    summed = jnp.dot(table, arrived, preferred_element_type=jnp.float32).astype(jnp.bfloat16)

    summed = exchange(summed, "grp")
    siblings = [[mate * planes + d for d in range(planes)] for mate in range(mates)]
    summed = exchange(summed, "ep", siblings)
    return summed.reshape(planes, TOK_DEV, strip).swapaxes(0, 1).reshape(TOK_DEV, width)


def solution(mesh):
    in_specs = (
        P("grp", "ep", None, None),
        P("ep", None, None),
        P("grp", "ep", None),
        P("grp", "ep", None),
        P("grp", "ep", None),
        P("grp", "ep", None),
    )
    out_specs = P(("grp", "ep"), None)
    return jax.shard_map(body, mesh=mesh, in_specs=in_specs, out_specs=out_specs, check_vma=False)
```

```python
import jax
import jax.numpy as jnp
from jax import lax
from jax.experimental import pallas as pl
from jax.experimental.pallas import tpu as pltpu
from jax.sharding import PartitionSpec as P

TOK_DEV = 32


def exchange(value, axis, groups=None):
    return lax.all_to_all(value, axis, split_axis=0, concat_axis=0, tiled=True, axis_index_groups=groups)


def moved(rows, source):
    pick = source == lax.broadcasted_iota(jnp.int32, source.shape, 1)
    pick = pick.astype(jnp.float32).astype(jnp.bfloat16)
    return jnp.dot(pick, rows, preferred_element_type=jnp.float32).astype(jnp.bfloat16)


def scale_kernel(planes, mates, send, gate_ref, count_ref, hidden_ref, out_ref):
    slots, columns = hidden_ref.shape[0], count_ref.shape[1]
    slot = lax.broadcasted_iota(jnp.int32, (slots, 1), 0)
    own = slot == lax.broadcasted_iota(jnp.int32, (slots, slots), 1)
    gate = jnp.sum(jnp.where(own, gate_ref[...], 0.0), axis=1, keepdims=True)
    block = slot // send == lax.broadcasted_iota(jnp.int32, (slots, columns), 1)
    limit = jnp.sum(jnp.where(block, count_ref[...], 0).astype(jnp.float32), axis=1, keepdims=True)
    scale = jnp.where((slot % send).astype(jnp.float32) < limit, gate, 0.0)
    scaled = (hidden_ref[...].astype(jnp.float32) * scale).astype(jnp.bfloat16)
    place = lax.broadcasted_iota(jnp.int32, (slots, slots), 0)
    plane, mate, slot = place // (mates * send), (place // send) % mates, place % send
    out_ref[...] = moved(scaled, (mate * planes + plane) * send + slot)


def scaled_rows(hidden, gate, count, planes, mates, send):
    return pl.pallas_call(
        lambda *refs: scale_kernel(planes, mates, send, *refs),
        out_shape=jax.ShapeDtypeStruct(hidden.shape, jnp.bfloat16),
        cost_estimate=pl.CostEstimate(flops=2 * hidden.size, bytes_accessed=4 * hidden.size, transcendentals=0),
        name="scaled_rows",
    )(gate, count, hidden)


def product_kernel(planes, mates, send, rows_ref, weight_ref, out_ref, weights, outs, in_sems, out_sems):
    count = rows_ref.shape[0]
    pieces, _, block = weights.shape
    strip = out_ref.shape[3]
    per = block // strip
    loads = [
        pltpu.make_async_copy(weight_ref.at[:, i * block : (i + 1) * block], weights.at[i], in_sems.at[i])
        for i in range(pieces)
    ]
    stores = [
        pltpu.make_async_copy(outs.at[:, i * per : (i + 1) * per], out_ref.at[:, i * per : (i + 1) * per], out_sems.at[i])
        for i in range(pieces)
    ]
    for load in loads:
        load.start()
    place = lax.broadcasted_iota(jnp.int32, (count, count), 0)
    mate, group, slot = place // (planes * send), (place // send) % planes, place % send
    rows = moved(rows_ref[...], (group * mates + mate) * send + slot)
    bundle = planes * send
    for i in range(pieces):
        loads[i].wait()
        product = jnp.dot(rows, weights[i], preferred_element_type=jnp.float32).astype(jnp.bfloat16)
        for j in range(per):
            for k in range(mates):
                outs[k, i * per + j] = product[k * bundle : (k + 1) * bundle, j * strip : (j + 1) * strip]
        if i:
            stores[i - 1].start()
    stores[-1].start()
    for store in stores:
        store.wait()


def strip_product(rows, weight, planes, mates, send):
    count, depth = rows.shape
    width = weight.shape[1]
    strip = width // planes
    block = 2 * strip
    pieces = width // block
    shape = (mates, planes, planes * send, strip)
    return pl.pallas_call(
        lambda *refs: product_kernel(planes, mates, send, *refs),
        out_shape=jax.ShapeDtypeStruct(shape, jnp.bfloat16),
        in_specs=[pl.BlockSpec(memory_space=pltpu.VMEM), pl.BlockSpec(memory_space=pltpu.HBM)],
        out_specs=pl.BlockSpec(memory_space=pltpu.HBM),
        scratch_shapes=[
            pltpu.VMEM((pieces, depth, block), jnp.bfloat16),
            pltpu.VMEM(shape, jnp.bfloat16),
            pltpu.SemaphoreType.DMA((pieces,)),
            pltpu.SemaphoreType.DMA((pieces,)),
        ],
        cost_estimate=pl.CostEstimate(
            flops=2 * count * depth * width, bytes_accessed=2 * (depth + count) * width, transcendentals=0
        ),
        compiler_params=pltpu.CompilerParams(vmem_limit_bytes=50 * 1024 * 1024),
        name="strip_product",
    )(rows, weight)


def gathered(index, pick):
    columns = lax.axis_size("ep")
    near = min(8, columns // 2)
    index, step, bits = index[None], columns // 2, 0
    while step >= near:
        upper = (lax.axis_index("ep") // step) % 2 == 1
        other = lax.ppermute(index, "ep", [(i, i ^ step) for i in range(columns)])
        low, high = jnp.where(upper, other, index), jnp.where(upper, index, other)
        index = jnp.concatenate([low, high], axis=0)
        step, bits = step // 2, bits + 1
    index = pick(index)
    groups = [[i * near + j for j in range(near)] for i in range(columns // near)]
    index = lax.all_gather(index, "ep", axis=0, axis_index_groups=groups)
    index = index.reshape((near,) + (2,) * bits + index.shape[2:])
    order = tuple(range(bits, 0, -1)) + (0,) + tuple(range(bits + 1, index.ndim))
    return index.transpose(order).reshape((columns,) + index.shape[bits + 1 :])


def body(hidden, down_weight, slot_gate, slot_owner, slot_row, block_count):
    planes = lax.axis_size("grp")
    columns = lax.axis_size("ep")
    slot_total = hidden.shape[2]
    width = down_weight.shape[2]
    mates = columns // planes
    send = slot_total // columns
    strip = width // planes

    rows = scaled_rows(hidden[0, 0], slot_gate[0], block_count[0], planes, mates, send)
    rows = exchange(rows, "grp")

    def own_mate(value):
        value = value.reshape(value.shape[0], mates, planes * send)
        return lax.dynamic_index_in_dim(value, lax.axis_index("ep") // planes, axis=1, keepdims=False)

    index = slot_owner[0, 0] * TOK_DEV + slot_row[0, 0]
    index = gathered(index, own_mate).reshape(columns, planes, send)
    index = index.swapaxes(0, 1).reshape(planes, columns * send)

    product = strip_product(rows, down_weight[0], planes, mates, send)
    arrived = exchange(product.reshape(columns * planes * send, strip), "ep")

    index = lax.all_gather(index, "grp", axis=0)
    index = lax.dynamic_index_in_dim(index, lax.axis_index("grp"), axis=1, keepdims=False)
    index = index.reshape(planes, columns, send).swapaxes(0, 1).reshape(-1)

    siblings = [[mate * planes + d for d in range(planes)] for mate in range(mates)]
    shift = [b // 2 + planes // 2 * (b % 2) for b in range(planes)]
    block = jnp.arange(planes)
    owner = (lax.axis_index("grp") + block // 2 + planes // 2 * (block % 2)) % planes
    wanted = (owner[:, None] * TOK_DEV + jnp.arange(TOK_DEV)[None, :]).reshape(-1)
    table = (wanted[:, None] == index[None, :]).astype(jnp.bfloat16)
    summed = jnp.dot(table, arrived, preferred_element_type=jnp.float32).astype(jnp.bfloat16)

    summed = exchange(summed, "ep", siblings)
    summed = summed.reshape(planes, TOK_DEV, strip).swapaxes(0, 1).reshape(TOK_DEV, width)
    route = [
        (z * columns + mate * planes + b, (z + shift[b]) % planes * columns + mate * planes + z)
        for z in range(planes)
        for mate in range(mates)
        for b in range(planes)
    ]
    return lax.ppermute(summed, ("grp", "ep"), route)


def solution(mesh):
    in_specs = (
        P("grp", "ep", None, None),
        P("ep", None, None),
        P("grp", "ep", None),
        P("grp", "ep", None),
        P("grp", "ep", None),
        P("grp", "ep", None),
    )
    out_specs = P(("grp", "ep"), None)
    return jax.shard_map(body, mesh=mesh, in_specs=in_specs, out_specs=out_specs, check_vma=False)
```

```python
import jax
import jax.numpy as jnp
from jax import lax
from jax.experimental import pallas as pl
from jax.experimental.pallas import tpu as pltpu
from jax.sharding import PartitionSpec as P

TOK_DEV = 32


def exchange(value, axis, groups=None):
    return lax.all_to_all(value, axis, split_axis=0, concat_axis=0, tiled=True, axis_index_groups=groups)


def moved(rows, source):
    pick = source == lax.broadcasted_iota(jnp.int32, source.shape, 1)
    pick = pick.astype(jnp.float32).astype(jnp.bfloat16)
    return jnp.dot(pick, rows, preferred_element_type=jnp.float32).astype(jnp.bfloat16)


def scale_kernel(planes, mates, send, gate_ref, count_ref, hidden_ref, out_ref, rows, sem):
    load = pltpu.make_async_copy(hidden_ref, rows, sem)
    load.start()
    slots, columns = rows.shape[0], count_ref.shape[1]
    slot = lax.broadcasted_iota(jnp.int32, (slots, 1), 0)
    own = slot == lax.broadcasted_iota(jnp.int32, (slots, slots), 1)
    gate = jnp.sum(jnp.where(own, gate_ref[...], 0.0), axis=1, keepdims=True)
    block = slot // send == lax.broadcasted_iota(jnp.int32, (slots, columns), 1)
    limit = jnp.sum(jnp.where(block, count_ref[...], 0).astype(jnp.float32), axis=1, keepdims=True)
    scale = jnp.where((slot % send).astype(jnp.float32) < limit, gate, 0.0)
    plane, mate, slot = slot // (mates * send), (slot // send) % mates, slot % send
    source = jnp.broadcast_to((mate * planes + plane) * send + slot, (slots, slots))
    load.wait()
    scaled = (rows[...].astype(jnp.float32) * scale).astype(jnp.bfloat16)
    out_ref[...] = moved(scaled, source)


def scaled_rows(hidden, gate, count, planes, mates, send):
    return pl.pallas_call(
        lambda *refs: scale_kernel(planes, mates, send, *refs),
        out_shape=jax.ShapeDtypeStruct(hidden.shape, jnp.bfloat16),
        in_specs=[
            pl.BlockSpec(memory_space=pltpu.VMEM),
            pl.BlockSpec(memory_space=pltpu.VMEM),
            pl.BlockSpec(memory_space=pltpu.HBM),
        ],
        scratch_shapes=[pltpu.VMEM(hidden.shape, hidden.dtype), pltpu.SemaphoreType.DMA],
        cost_estimate=pl.CostEstimate(flops=2 * hidden.size, bytes_accessed=4 * hidden.size, transcendentals=0),
        name="scaled_rows",
    )(gate, count, hidden)


def product_kernel(planes, mates, send, rows_ref, weight_ref, out_ref, weights, outs, in_sems, out_sems):
    count = rows_ref.shape[0]
    pieces, _, block = weights.shape
    strip = out_ref.shape[3]
    per = block // strip
    loads = [
        pltpu.make_async_copy(weight_ref.at[:, i * block : (i + 1) * block], weights.at[i], in_sems.at[i])
        for i in range(pieces)
    ]
    stores = [
        pltpu.make_async_copy(outs.at[:, i * per : (i + 1) * per], out_ref.at[:, i * per : (i + 1) * per], out_sems.at[i])
        for i in range(pieces)
    ]
    for load in loads:
        load.start()
    place = lax.broadcasted_iota(jnp.int32, (count, 1), 0)
    mate, group, slot = place // (planes * send), (place // send) % planes, place % send
    source = jnp.broadcast_to((group * mates + mate) * send + slot, (count, count))
    rows = moved(rows_ref[...], source)
    bundle = planes * send
    for i in range(pieces):
        loads[i].wait()
        product = jnp.dot(rows, weights[i], preferred_element_type=jnp.float32).astype(jnp.bfloat16)
        for j in range(per):
            for k in range(mates):
                outs[k, i * per + j] = product[k * bundle : (k + 1) * bundle, j * strip : (j + 1) * strip]
        if i:
            stores[i - 1].start()
    stores[-1].start()
    for store in stores:
        store.wait()


def strip_product(rows, weight, planes, mates, send):
    count, depth = rows.shape
    width = weight.shape[1]
    strip = width // planes
    block = 2 * strip
    pieces = width // block
    shape = (mates, planes, planes * send, strip)
    return pl.pallas_call(
        lambda *refs: product_kernel(planes, mates, send, *refs),
        out_shape=jax.ShapeDtypeStruct(shape, jnp.bfloat16),
        in_specs=[pl.BlockSpec(memory_space=pltpu.VMEM), pl.BlockSpec(memory_space=pltpu.HBM)],
        out_specs=pl.BlockSpec(memory_space=pltpu.HBM),
        scratch_shapes=[
            pltpu.VMEM((pieces, depth, block), jnp.bfloat16),
            pltpu.VMEM(shape, jnp.bfloat16),
            pltpu.SemaphoreType.DMA((pieces,)),
            pltpu.SemaphoreType.DMA((pieces,)),
        ],
        cost_estimate=pl.CostEstimate(
            flops=2 * count * depth * width, bytes_accessed=2 * (depth + count) * width, transcendentals=0
        ),
        compiler_params=pltpu.CompilerParams(vmem_limit_bytes=50 * 1024 * 1024),
        name="strip_product",
    )(rows, weight)


def gathered(index, pick):
    columns = lax.axis_size("ep")
    near = min(8, columns // 2)
    index, step, bits = index[None], columns // 2, 0
    while step >= near:
        upper = (lax.axis_index("ep") // step) % 2 == 1
        other = lax.ppermute(index, "ep", [(i, i ^ step) for i in range(columns)])
        low, high = jnp.where(upper, other, index), jnp.where(upper, index, other)
        index = jnp.concatenate([low, high], axis=0)
        step, bits = step // 2, bits + 1
    index = pick(index)
    groups = [[i * near + j for j in range(near)] for i in range(columns // near)]
    index = lax.all_gather(index, "ep", axis=0, axis_index_groups=groups)
    index = index.reshape((near,) + (2,) * bits + index.shape[2:])
    order = tuple(range(bits, 0, -1)) + (0,) + tuple(range(bits + 1, index.ndim))
    return index.transpose(order).reshape((columns,) + index.shape[bits + 1 :])


def body(hidden, down_weight, slot_gate, slot_owner, slot_row, block_count):
    planes = lax.axis_size("grp")
    columns = lax.axis_size("ep")
    slot_total = hidden.shape[2]
    width = down_weight.shape[2]
    mates = columns // planes
    send = slot_total // columns
    strip = width // planes

    rows = scaled_rows(hidden[0, 0], slot_gate[0], block_count[0], planes, mates, send)
    rows = exchange(rows, "grp")

    def own_mate(value):
        value = value.reshape(value.shape[0], mates, planes * send)
        return lax.dynamic_index_in_dim(value, lax.axis_index("ep") // planes, axis=1, keepdims=False)

    index = slot_owner[0, 0] * TOK_DEV + slot_row[0, 0]
    index = gathered(index, own_mate).reshape(columns, planes, send)
    index = index.swapaxes(0, 1).reshape(planes, columns * send)

    product = strip_product(rows, down_weight[0], planes, mates, send)
    arrived = exchange(product.reshape(columns * planes * send, strip), "ep")

    index = lax.all_gather(index, "grp", axis=0)
    index = lax.dynamic_index_in_dim(index, lax.axis_index("grp"), axis=1, keepdims=False)
    index = index.reshape(planes, columns, send).swapaxes(0, 1).reshape(-1)

    wanted = jnp.arange(planes * TOK_DEV)
    table = (wanted[:, None] == index[None, :]).astype(jnp.bfloat16)
    summed = jnp.dot(table, arrived, preferred_element_type=jnp.float32).astype(jnp.bfloat16)

    summed = exchange(summed, "grp")
    siblings = [[mate * planes + d for d in range(planes)] for mate in range(mates)]
    summed = exchange(summed, "ep", siblings)
    return summed.reshape(planes, TOK_DEV, strip).swapaxes(0, 1).reshape(TOK_DEV, width)


def solution(mesh):
    in_specs = (
        P("grp", "ep", None, None),
        P("ep", None, None),
        P("grp", "ep", None),
        P("grp", "ep", None),
        P("grp", "ep", None),
        P("grp", "ep", None),
    )
    out_specs = P(("grp", "ep"), None)
    return jax.shard_map(body, mesh=mesh, in_specs=in_specs, out_specs=out_specs, check_vma=False)
```

```python
import jax
import jax.numpy as jnp
from jax import lax
from jax.experimental import pallas as pl
from jax.experimental.pallas import tpu as pltpu
from jax.sharding import PartitionSpec as P

TOK_DEV = 32


def exchange(value, axis, groups=None):
    return lax.all_to_all(value, axis, split_axis=0, concat_axis=0, tiled=True, axis_index_groups=groups)


def moved(rows, source):
    pick = source == lax.broadcasted_iota(jnp.int32, source.shape, 1)
    pick = pick.astype(jnp.float32).astype(jnp.bfloat16)
    return jnp.dot(pick, rows, preferred_element_type=jnp.float32).astype(jnp.bfloat16)


def scale_kernel(planes, mates, send, gate_ref, count_ref, hidden_ref, out_ref):
    slots, columns = hidden_ref.shape[0], count_ref.shape[1]
    slot = lax.broadcasted_iota(jnp.int32, (slots, 1), 0)
    own = slot == lax.broadcasted_iota(jnp.int32, (slots, slots), 1)
    gate = jnp.sum(jnp.where(own, gate_ref[...], 0.0), axis=1, keepdims=True)
    block = slot // send == lax.broadcasted_iota(jnp.int32, (slots, columns), 1)
    limit = jnp.sum(jnp.where(block, count_ref[...], 0).astype(jnp.float32), axis=1, keepdims=True)
    scale = jnp.where((slot % send).astype(jnp.float32) < limit, gate, 0.0)
    plane, mate, slot = slot // (mates * send), (slot // send) % mates, slot % send
    source = jnp.broadcast_to((mate * planes + plane) * send + slot, (slots, slots))
    scaled = (hidden_ref[...].astype(jnp.float32) * scale).astype(jnp.bfloat16)
    out_ref[...] = moved(scaled, source)


def scaled_rows(hidden, gate, count, planes, mates, send):
    return pl.pallas_call(
        lambda *refs: scale_kernel(planes, mates, send, *refs),
        out_shape=jax.ShapeDtypeStruct(hidden.shape, jnp.bfloat16),
        cost_estimate=pl.CostEstimate(flops=2 * hidden.size, bytes_accessed=4 * hidden.size, transcendentals=0),
        name="scaled_rows",
    )(gate, count, hidden)


def product_kernel(planes, mates, send, rows_ref, weight_ref, out_ref, weights, outs, in_sems, out_sems):
    count = rows_ref.shape[0]
    pieces, _, block = weights.shape
    strip = out_ref.shape[3]
    per = block // strip
    loads = [
        pltpu.make_async_copy(weight_ref.at[:, i * block : (i + 1) * block], weights.at[i], in_sems.at[i])
        for i in range(pieces)
    ]
    stores = [
        pltpu.make_async_copy(outs.at[:, i * per : (i + 1) * per], out_ref.at[:, i * per : (i + 1) * per], out_sems.at[i])
        for i in range(pieces)
    ]
    for load in loads:
        load.start()
    place = lax.broadcasted_iota(jnp.int32, (count, 1), 0)
    mate, group, slot = place // (planes * send), (place // send) % planes, place % send
    source = jnp.broadcast_to((group * mates + mate) * send + slot, (count, count))
    rows = moved(rows_ref[...], source)
    bundle = planes * send
    for i in range(pieces):
        loads[i].wait()
        product = jnp.dot(rows, weights[i], preferred_element_type=jnp.float32).astype(jnp.bfloat16)
        for j in range(per):
            for k in range(mates):
                outs[k, i * per + j] = product[k * bundle : (k + 1) * bundle, j * strip : (j + 1) * strip]
        if i:
            stores[i - 1].start()
    stores[-1].start()
    for store in stores:
        store.wait()


def strip_product(rows, weight, planes, mates, send):
    count, depth = rows.shape
    width = weight.shape[1]
    strip = width // planes
    block = 2 * strip
    pieces = width // block
    shape = (mates, planes, planes * send, strip)
    return pl.pallas_call(
        lambda *refs: product_kernel(planes, mates, send, *refs),
        out_shape=jax.ShapeDtypeStruct(shape, jnp.bfloat16),
        in_specs=[pl.BlockSpec(memory_space=pltpu.VMEM), pl.BlockSpec(memory_space=pltpu.HBM)],
        out_specs=pl.BlockSpec(memory_space=pltpu.HBM),
        scratch_shapes=[
            pltpu.VMEM((pieces, depth, block), jnp.bfloat16),
            pltpu.VMEM(shape, jnp.bfloat16),
            pltpu.SemaphoreType.DMA((pieces,)),
            pltpu.SemaphoreType.DMA((pieces,)),
        ],
        cost_estimate=pl.CostEstimate(
            flops=2 * count * depth * width, bytes_accessed=2 * (depth + count) * width, transcendentals=0
        ),
        compiler_params=pltpu.CompilerParams(vmem_limit_bytes=50 * 1024 * 1024),
        name="strip_product",
    )(rows, weight)


def doubled(index, near):
    columns = lax.axis_size("ep")
    step, bits = columns // 2, 0
    while step >= near:
        upper = (lax.axis_index("ep") // step) % 2 == 1
        other = lax.ppermute(index, "ep", [(i, i ^ step) for i in range(columns)])
        low, high = jnp.where(upper, other, index), jnp.where(upper, index, other)
        index = jnp.stack([low, high], axis=0)
        step, bits = step // 2, bits + 1
    return index, bits


def body(hidden, down_weight, slot_gate, slot_owner, slot_row, block_count):
    planes = lax.axis_size("grp")
    columns = lax.axis_size("ep")
    slot_total = hidden.shape[2]
    width = down_weight.shape[2]
    mates = columns // planes
    send = slot_total // columns
    strip = width // planes

    rows = scaled_rows(hidden[0, 0], slot_gate[0], block_count[0], planes, mates, send)
    rows = exchange(rows, "grp")

    near = min(8, columns // 2)
    index = slot_owner[0, 0] * TOK_DEV + slot_row[0, 0]
    index, bits = doubled(index, near)
    index = index.reshape(columns // near, mates, planes, send)
    index = lax.dynamic_index_in_dim(index, lax.axis_index("ep") // planes, axis=1, keepdims=False)
    index = index.swapaxes(0, 1).reshape(planes, columns // near * send)

    rows, index = lax.optimization_barrier((rows, index))
    product = strip_product(rows, down_weight[0], planes, mates, send)
    arrived = exchange(product.reshape(columns * planes * send, strip), "ep")

    index = lax.all_gather(index, "grp", axis=0)
    index = lax.dynamic_index_in_dim(index, lax.axis_index("grp"), axis=1, keepdims=False)
    groups = [[i * near + j for j in range(near)] for i in range(columns // near)]
    index = lax.all_gather(index, "ep", axis=0, axis_index_groups=groups)
    index = index.reshape((near, planes) + (2,) * bits + (send,))
    order = tuple(range(bits + 1, 1, -1)) + (0, 1, bits + 2)
    index = index.transpose(order).reshape(-1)

    wanted = jnp.arange(planes * TOK_DEV)
    table = (wanted[:, None] == index[None, :]).astype(jnp.bfloat16)
    summed = jnp.dot(table, arrived, preferred_element_type=jnp.float32).astype(jnp.bfloat16)

    summed = exchange(summed, "grp")
    siblings = [[mate * planes + d for d in range(planes)] for mate in range(mates)]
    summed = exchange(summed, "ep", siblings)
    return summed.reshape(planes, TOK_DEV, strip).swapaxes(0, 1).reshape(TOK_DEV, width)


def solution(mesh):
    in_specs = (
        P("grp", "ep", None, None),
        P("ep", None, None),
        P("grp", "ep", None),
        P("grp", "ep", None),
        P("grp", "ep", None),
        P("grp", "ep", None),
    )
    out_specs = P(("grp", "ep"), None)
    return jax.shard_map(body, mesh=mesh, in_specs=in_specs, out_specs=out_specs, check_vma=False)
```

```python
import jax
import jax.numpy as jnp
from jax import lax
from jax.experimental import pallas as pl
from jax.experimental.pallas import tpu as pltpu
from jax.sharding import PartitionSpec as P

TOK_DEV = 32
STRIDE = 3


def exchange(value, axis, groups=None):
    return lax.all_to_all(value, axis, split_axis=0, concat_axis=0, tiled=True, axis_index_groups=groups)


def moved(rows, source):
    pick = source == lax.broadcasted_iota(jnp.int32, source.shape, 1)
    pick = pick.astype(jnp.float32).astype(jnp.bfloat16)
    return jnp.dot(pick, rows, preferred_element_type=jnp.float32).astype(jnp.bfloat16)


def scale_kernel(planes, mates, send, gate_ref, count_ref, hidden_ref, out_ref):
    slots, columns = hidden_ref.shape[0], count_ref.shape[1]
    slot = lax.broadcasted_iota(jnp.int32, (slots, 1), 0)
    own = slot == lax.broadcasted_iota(jnp.int32, (slots, slots), 1)
    gate = jnp.sum(jnp.where(own, gate_ref[...], 0.0), axis=1, keepdims=True)
    block = slot // send == lax.broadcasted_iota(jnp.int32, (slots, columns), 1)
    limit = jnp.sum(jnp.where(block, count_ref[...], 0).astype(jnp.float32), axis=1, keepdims=True)
    scale = jnp.where((slot % send).astype(jnp.float32) < limit, gate, 0.0)
    plane = slot // (mates * send) * pow(STRIDE, -1, planes) % planes
    mate, slot = (slot // send) % mates, slot % send
    source = jnp.broadcast_to((mate * planes + plane) * send + slot, (slots, slots))
    scaled = (hidden_ref[...].astype(jnp.float32) * scale).astype(jnp.bfloat16)
    out_ref[...] = moved(scaled, source)


def scaled_rows(hidden, gate, count, planes, mates, send):
    return pl.pallas_call(
        lambda *refs: scale_kernel(planes, mates, send, *refs),
        out_shape=jax.ShapeDtypeStruct(hidden.shape, jnp.bfloat16),
        cost_estimate=pl.CostEstimate(flops=2 * hidden.size, bytes_accessed=4 * hidden.size, transcendentals=0),
        name="scaled_rows",
    )(gate, count, hidden)


def product_kernel(planes, mates, send, rows_ref, weight_ref, out_ref, weights, outs, in_sems, out_sems):
    count = rows_ref.shape[0]
    pieces, _, block = weights.shape
    strip = out_ref.shape[3]
    per = block // strip
    loads = [
        pltpu.make_async_copy(weight_ref.at[:, i * block : (i + 1) * block], weights.at[i], in_sems.at[i])
        for i in range(pieces)
    ]
    homes = [i * STRIDE % planes for i in range(planes)]
    stores = [pltpu.make_async_copy(outs.at[:, i], out_ref.at[:, i], out_sems.at[i]) for i in homes]
    for load in loads:
        load.start()
    place = lax.broadcasted_iota(jnp.int32, (count, 1), 0)
    mate, group, slot = place // (planes * send), (place // send) % planes, place % send
    group = group * STRIDE % planes
    source = jnp.broadcast_to((group * mates + mate) * send + slot, (count, count))
    rows = moved(rows_ref[...], source)
    bundle = planes * send
    for i in range(pieces):
        loads[i].wait()
        product = jnp.dot(rows, weights[i], preferred_element_type=jnp.float32).astype(jnp.bfloat16)
        for j in range(per):
            for k in range(mates):
                outs[k, homes[i * per + j]] = product[k * bundle : (k + 1) * bundle, j * strip : (j + 1) * strip]
        for store in stores[(i - 1) * per : i * per] if i else ():
            store.start()
    for store in stores[-per:]:
        store.start()
    for store in stores:
        store.wait()


def strip_product(rows, weight, planes, mates, send):
    count, depth = rows.shape
    width = weight.shape[1]
    strip = width // planes
    block = 2 * strip
    pieces = width // block
    shape = (mates, planes, planes * send, strip)
    return pl.pallas_call(
        lambda *refs: product_kernel(planes, mates, send, *refs),
        out_shape=jax.ShapeDtypeStruct(shape, jnp.bfloat16),
        in_specs=[pl.BlockSpec(memory_space=pltpu.VMEM), pl.BlockSpec(memory_space=pltpu.HBM)],
        out_specs=pl.BlockSpec(memory_space=pltpu.HBM),
        scratch_shapes=[
            pltpu.VMEM((pieces, depth, block), jnp.bfloat16),
            pltpu.VMEM(shape, jnp.bfloat16),
            pltpu.SemaphoreType.DMA((pieces,)),
            pltpu.SemaphoreType.DMA((planes,)),
        ],
        cost_estimate=pl.CostEstimate(
            flops=2 * count * depth * width, bytes_accessed=2 * (depth + count) * width, transcendentals=0
        ),
        compiler_params=pltpu.CompilerParams(vmem_limit_bytes=50 * 1024 * 1024),
        name="strip_product",
    )(rows, weight)


def doubled(index, near):
    columns = lax.axis_size("ep")
    step, bits = columns // 2, 0
    while step >= near:
        upper = (lax.axis_index("ep") // step) % 2 == 1
        other = lax.ppermute(index, "ep", [(i, i ^ step) for i in range(columns)])
        low, high = jnp.where(upper, other, index), jnp.where(upper, index, other)
        index = jnp.stack([low, high], axis=0)
        step, bits = step // 2, bits + 1
    return index, bits


def body(hidden, down_weight, slot_gate, slot_owner, slot_row, block_count):
    planes = lax.axis_size("grp")
    columns = lax.axis_size("ep")
    slot_total = hidden.shape[2]
    width = down_weight.shape[2]
    mates = columns // planes
    send = slot_total // columns
    strip = width // planes

    rows = scaled_rows(hidden[0, 0], slot_gate[0], block_count[0], planes, mates, send)
    rows = exchange(rows, "grp", [[i * pow(STRIDE, -1, planes) % planes for i in range(planes)]])

    near = min(8, columns // 2)
    index = slot_owner[0, 0] * TOK_DEV + slot_row[0, 0]
    index, bits = doubled(index, near)
    index = index.reshape(columns // near, mates, planes, send)
    index = lax.dynamic_index_in_dim(index, lax.axis_index("ep") // planes, axis=1, keepdims=False)
    index = index.swapaxes(0, 1).reshape(planes, columns // near * send)

    rows, index = lax.optimization_barrier((rows, index))
    product = strip_product(rows, down_weight[0], planes, mates, send)
    arrived = exchange(product.reshape(columns * planes * send, strip), "ep")

    index = lax.all_gather(index, "grp", axis=0)
    index = lax.dynamic_index_in_dim(index, lax.axis_index("grp"), axis=1, keepdims=False)
    groups = [[i * near + j for j in range(near)] for i in range(columns // near)]
    index = lax.all_gather(index, "ep", axis=0, axis_index_groups=groups)
    index = index.reshape((near, planes) + (2,) * bits + (send,))
    order = tuple(range(bits + 1, 1, -1)) + (0, 1, bits + 2)
    index = index.transpose(order).reshape(-1)

    order = [i * STRIDE % planes for i in range(planes)]
    place = jnp.arange(planes) * STRIDE % planes
    wanted = (place[:, None] * TOK_DEV + jnp.arange(TOK_DEV)[None, :]).reshape(-1)
    table = (wanted[:, None] == index[None, :]).astype(jnp.bfloat16)
    summed = jnp.dot(table, arrived, preferred_element_type=jnp.float32).astype(jnp.bfloat16)

    summed = exchange(summed, "grp", [order])
    siblings = [[mate * planes + d for d in order] for mate in range(mates)]
    summed = exchange(summed, "ep", siblings)
    return summed.reshape(planes, TOK_DEV, strip).swapaxes(0, 1).reshape(TOK_DEV, width)


def solution(mesh):
    in_specs = (
        P("grp", "ep", None, None),
        P("ep", None, None),
        P("grp", "ep", None),
        P("grp", "ep", None),
        P("grp", "ep", None),
        P("grp", "ep", None),
    )
    out_specs = P(("grp", "ep"), None)
    return jax.shard_map(body, mesh=mesh, in_specs=in_specs, out_specs=out_specs, check_vma=False)
```

```python
import jax
import jax.numpy as jnp
from jax import lax
from jax.experimental import pallas as pl
from jax.experimental.pallas import tpu as pltpu
from jax.sharding import PartitionSpec as P

TOK_DEV = 32
STRIDE = 11


def exchange(value, axis, groups=None):
    return lax.all_to_all(value, axis, split_axis=0, concat_axis=0, tiled=True, axis_index_groups=groups)


def moved(rows, source):
    pick = source == lax.broadcasted_iota(jnp.int32, source.shape, 1)
    pick = pick.astype(jnp.float32).astype(jnp.bfloat16)
    return jnp.dot(pick, rows, preferred_element_type=jnp.float32).astype(jnp.bfloat16)


def scale_kernel(planes, mates, send, gate_ref, count_ref, hidden_ref, out_ref):
    slots, columns = hidden_ref.shape[0], count_ref.shape[1]
    slot = lax.broadcasted_iota(jnp.int32, (slots, 1), 0)
    own = slot == lax.broadcasted_iota(jnp.int32, (slots, slots), 1)
    gate = jnp.sum(jnp.where(own, gate_ref[...], 0.0), axis=1, keepdims=True)
    block = slot // send == lax.broadcasted_iota(jnp.int32, (slots, columns), 1)
    limit = jnp.sum(jnp.where(block, count_ref[...], 0).astype(jnp.float32), axis=1, keepdims=True)
    scale = jnp.where((slot % send).astype(jnp.float32) < limit, gate, 0.0)
    plane = slot // (mates * send) * STRIDE % planes
    mate, slot = (slot // send) % mates, slot % send
    source = jnp.broadcast_to((mate * planes + plane) * send + slot, (slots, slots))
    scaled = (hidden_ref[...].astype(jnp.float32) * scale).astype(jnp.bfloat16)
    out_ref[...] = moved(scaled, source)


def scaled_rows(hidden, gate, count, planes, mates, send):
    return pl.pallas_call(
        lambda *refs: scale_kernel(planes, mates, send, *refs),
        out_shape=jax.ShapeDtypeStruct(hidden.shape, jnp.bfloat16),
        cost_estimate=pl.CostEstimate(flops=2 * hidden.size, bytes_accessed=4 * hidden.size, transcendentals=0),
        name="scaled_rows",
    )(gate, count, hidden)


def product_kernel(planes, mates, send, rows_ref, weight_ref, out_ref, weights, outs, in_sems, out_sems):
    count = rows_ref.shape[0]
    pieces, _, block = weights.shape
    strip = out_ref.shape[3]
    per = block // strip
    loads = [
        pltpu.make_async_copy(weight_ref.at[:, i * block : (i + 1) * block], weights.at[i], in_sems.at[i])
        for i in range(pieces)
    ]
    stores = [pltpu.make_async_copy(outs.at[:, i], out_ref.at[:, i], out_sems.at[i]) for i in range(planes)]
    for load in loads:
        load.start()
    place = lax.broadcasted_iota(jnp.int32, (count, 1), 0)
    mate, group, slot = place // (planes * send), (place // send) % planes, place % send
    group = group * pow(STRIDE, -1, planes) % planes
    source = jnp.broadcast_to((group * mates + mate) * send + slot, (count, count))
    rows = moved(rows_ref[...], source)
    bundle = planes * send
    for i in range(pieces):
        loads[i].wait()
        product = jnp.dot(rows, weights[i], preferred_element_type=jnp.float32).astype(jnp.bfloat16)
        for j in range(per):
            for k in range(mates):
                outs[k, i * per + j] = product[k * bundle : (k + 1) * bundle, j * strip : (j + 1) * strip]
        for store in stores[(i - 1) * per : i * per] if i else ():
            store.start()
    for store in stores[-per:]:
        store.start()
    for store in stores:
        store.wait()


def strip_product(rows, weight, planes, mates, send):
    count, depth = rows.shape
    width = weight.shape[1]
    strip = width // planes
    block = 4 * strip
    pieces = width // block
    shape = (mates, planes, planes * send, strip)
    return pl.pallas_call(
        lambda *refs: product_kernel(planes, mates, send, *refs),
        out_shape=jax.ShapeDtypeStruct(shape, jnp.bfloat16),
        in_specs=[pl.BlockSpec(memory_space=pltpu.VMEM), pl.BlockSpec(memory_space=pltpu.HBM)],
        out_specs=pl.BlockSpec(memory_space=pltpu.HBM),
        scratch_shapes=[
            pltpu.VMEM((pieces, depth, block), jnp.bfloat16),
            pltpu.VMEM(shape, jnp.bfloat16),
            pltpu.SemaphoreType.DMA((pieces,)),
            pltpu.SemaphoreType.DMA((planes,)),
        ],
        cost_estimate=pl.CostEstimate(
            flops=2 * count * depth * width, bytes_accessed=2 * (depth + count) * width, transcendentals=0
        ),
        compiler_params=pltpu.CompilerParams(vmem_limit_bytes=50 * 1024 * 1024),
        name="strip_product",
    )(rows, weight)


def doubled(index, near):
    columns = lax.axis_size("ep")
    step, bits = columns // 2, 0
    while step >= near:
        upper = (lax.axis_index("ep") // step) % 2 == 1
        other = lax.ppermute(index, "ep", [(i, i ^ step) for i in range(columns)])
        low, high = jnp.where(upper, other, index), jnp.where(upper, index, other)
        index = jnp.stack([low, high], axis=0)
        step, bits = step // 2, bits + 1
    return index, bits


def body(hidden, down_weight, slot_gate, slot_owner, slot_row, block_count):
    planes = lax.axis_size("grp")
    columns = lax.axis_size("ep")
    slot_total = hidden.shape[2]
    width = down_weight.shape[2]
    mates = columns // planes
    send = slot_total // columns
    strip = width // planes

    rows = scaled_rows(hidden[0, 0], slot_gate[0], block_count[0], planes, mates, send)
    rows = exchange(rows, "grp", [[i * STRIDE % planes for i in range(planes)]])

    near = min(8, columns // 2)
    index = slot_owner[0, 0] * TOK_DEV + slot_row[0, 0]
    index, bits = doubled(index, near)
    index = index.reshape(columns // near, mates, planes, send)
    index = lax.dynamic_index_in_dim(index, lax.axis_index("ep") // planes, axis=1, keepdims=False)
    index = index.swapaxes(0, 1).reshape(planes, columns // near * send)

    rows, index = lax.optimization_barrier((rows, index))
    product = strip_product(rows, down_weight[0], planes, mates, send)
    arrived = exchange(product.reshape(columns * planes * send, strip), "ep")

    index = lax.all_gather(index, "grp", axis=0)
    index = lax.dynamic_index_in_dim(index, lax.axis_index("grp"), axis=1, keepdims=False)
    groups = [[i * near + j for j in range(near)] for i in range(columns // near)]
    index = lax.all_gather(index, "ep", axis=0, axis_index_groups=groups)
    index = index.reshape((near, planes) + (2,) * bits + (send,))
    order = tuple(range(bits + 1, 1, -1)) + (0, 1, bits + 2)
    index = index.transpose(order).reshape(-1)

    wanted = jnp.arange(planes * TOK_DEV)
    table = (wanted[:, None] == index[None, :]).astype(jnp.bfloat16)
    summed = jnp.dot(table, arrived, preferred_element_type=jnp.float32).astype(jnp.bfloat16)

    summed = exchange(summed, "grp")
    siblings = [[mate * planes + d for d in range(planes)] for mate in range(mates)]
    summed = exchange(summed, "ep", siblings)
    return summed.reshape(planes, TOK_DEV, strip).swapaxes(0, 1).reshape(TOK_DEV, width)


def solution(mesh):
    in_specs = (
        P("grp", "ep", None, None),
        P("ep", None, None),
        P("grp", "ep", None),
        P("grp", "ep", None),
        P("grp", "ep", None),
        P("grp", "ep", None),
    )
    out_specs = P(("grp", "ep"), None)
    return jax.shard_map(body, mesh=mesh, in_specs=in_specs, out_specs=out_specs, check_vma=False)
```
